128 devices in a mesh: scen: 32 (over x, z, core), blk: 4 (over y).
Axes of the slice: x: 4, y: 4, z: 4, core: 2. Of those that a mesh axis runs over, the one named last changes fastest.
Arguments:
- cons_matrix: bfloat16 [2048, 4096], P(None, 'blk'), may hold values from -0.09375 to 0.09375
- row_scale: float32 [2048, 2048], P('scen'), may hold values from 0.5 to 2
- rhs: float32 [2048, 2048], P('scen'), may hold values from -6 to 6
- cons_mult: float32 [2048, 2048], P('scen'), may hold values from -3 to 3
- cost: float32 [2048, 4096], P('scen', 'blk'), may hold values from -6 to 6
- ph_mult: float32 [2048, 4096], P('scen', 'blk'), may hold values from -3 to 3
- start: float32 [2048, 4096], P('scen', 'blk'), may hold values from -3 to 3
- consensus: float32 [4096], P('blk'), may hold values from -3 to 3
- upper: float32 [4096], P('blk'), may hold values from 0.3 to 1.5
- prob: float32 [2048], P('scen'), may hold values from 1 to 30, as said below
Outputs:
- solutions: float32 [2048, 4096], P('scen', 'blk')
- mult_new: float32 [2048, 2048], P('scen', 'blk')
- z_new: float32 [4096], P('blk')
- w_new: float32 [2048, 4096], P('scen', 'blk')
- primal_res: float32 [], replicated
- dual_res: float32 [], replicated
The draws below stay inside these ranges and needn't reach their ends.
Inputs may be any that keep to these rules, and one draw needn't show every extreme that they name: prob is positive.
All inputs are finite; a program needn't handle non-finite values.
Results may differ from the reference program's by a relative error of at most 0.0017.
Values may be sent and summed in bfloat16 or wider, within the bound.
No kernel may reach another device: no remote copies, remote signals or barrier semaphores. Data moves between devices by JAX's collectives and lax.ppermute only.
A program may use at most 64 MiB of HBM per device.

```python
import math
import jax
import jax.numpy as jnp
from jax import lax

M = 2048
NV = 4096
ITERS = 8
SCEN = 2048


def draw_prob(key, part):
    index = jnp.arange(SCEN).astype(jnp.float32)
    base = jnp.exp(jnp.log(3.0) * index / max(SCEN - 1, 1))
    noise = jax.random.uniform(key, (SCEN,), jnp.float32, 1.0, 3.0)
    return (base * noise).astype(jnp.float32)


def steps_of(stream_key, dims, cuts, low, largest):
    def one(dim, shards_of):
        steps = jax.random.uniform(jax.random.fold_in(jax.random.fold_in(stream_key, 6), dim), (shards_of,), jnp.float32, low / len(cuts), largest / len(cuts))
        return jnp.repeat(jnp.exp(steps), dims[dim] // shards_of).reshape((-1,) + (1,) * (len(dims) - dim - 1))

    factor_of = one(*cuts[0])
    for cut in cuts[1:]:
        factor_of = factor_of * one(*cut)
    return factor_of


def gaussian(own_key, extent, scale, bound, cuts=(), dtype=jnp.bfloat16):
    result = jax.random.normal(own_key, extent, jnp.float32) * scale
    if len(cuts) > 0:
        result = steps_of(own_key, extent, cuts, -0.22, 0.18) * result
    return jnp.clip(result, min=-bound, max=bound).astype(dtype)


def setup_inputs(seed: int = 0) -> dict:
    seeds = jax.random.split(jax.random.key(seed), 11)
    cons_matrix = gaussian(seeds[0], (M, NV), NV ** -0.5, 0.09375, ((1, 4),))
    row_scale = jnp.clip(jnp.exp(math.log(2.0) - 1.3862944 * jax.random.uniform(seeds[1], (SCEN, M), jnp.float32) ** steps_of(seeds[1], (SCEN, M), ((0, 32),), -0.2, 0.2)), 0.5, 2.0)
    rhs = gaussian(seeds[2], (SCEN, M), 1.0, 6.0, ((0, 32),), jnp.float32)
    cons_mult = gaussian(seeds[3], (SCEN, M), 0.5, 3.0, ((0, 32),), jnp.float32)
    cost = gaussian(seeds[4], (SCEN, NV), 1.0, 6.0, ((0, 32), (1, 4)), jnp.float32)
    ph_mult = gaussian(seeds[5], (SCEN, NV), 0.5, 3.0, ((0, 32), (1, 4)), jnp.float32)
    start = gaussian(seeds[6], (SCEN, NV), 0.5, 3.0, ((0, 32), (1, 4)), jnp.float32)
    consensus = gaussian(seeds[7], (NV,), 0.5, 3.0, ((0, 4),), jnp.float32)
    upper = jnp.clip(0.3 + 1.2 * jax.random.uniform(seeds[8], (NV,), jnp.float32) ** steps_of(seeds[8], (NV,), ((0, 4),), -0.2, 0.2), 0.3, 1.5)
    prob = draw_prob(jax.random.fold_in(seeds[10], 71), 0)
    return dict(cons_matrix=cons_matrix, row_scale=row_scale, rhs=rhs, cons_mult=cons_mult, cost=cost, ph_mult=ph_mult, start=start, consensus=consensus, upper=upper, prob=prob)


penalty = 1.0
aug_weight = 1.0
step_size = 0.05
eps = 1e-06

def reference(cons_matrix, row_scale, rhs, cons_mult, cost, ph_mult, start, consensus, upper, prob):
    x_now = start
    for step in range(ITERS):
        prod = jnp.dot(x_now.astype(jnp.bfloat16), cons_matrix.T, preferred_element_type=jnp.float32)
        weighted = (row_scale * (cons_mult + aug_weight * (row_scale * prod - rhs))).astype(jnp.bfloat16)
        back = jnp.dot(weighted, cons_matrix, preferred_element_type=jnp.float32)
        grad = cost + ph_mult + penalty * (x_now - consensus[None, :]) + back
        x_now = jnp.clip(x_now - step_size * grad, -upper[None, :], upper[None, :])
    prod_end = jnp.dot(x_now.astype(jnp.bfloat16), cons_matrix.T, preferred_element_type=jnp.float32)
    mult_new = cons_mult + aug_weight * (row_scale * prod_end - rhs)
    total = jnp.sum(prob)
    z_new = lax.optimization_barrier(jnp.sum(prob[:, None] * x_now, axis=0)) / total
    w_new = ph_mult + penalty * (x_now - z_new[None, :])
    primal_res = jnp.sqrt(jnp.sum(prob[:, None] * (x_now - z_new[None, :]) ** 2) / (total * NV) + eps)
    dual_res = penalty * jnp.sqrt(jnp.sum((z_new - consensus) ** 2) / NV + eps)
    return (x_now, mult_new, z_new, w_new, primal_res, dual_res)
```

```python
import functools

import jax
import jax.numpy as jnp
from jax import lax
from jax.experimental import pallas as pl
from jax.experimental.pallas import tpu as pltpu
from jax.sharding import Mesh
from jax.sharding import PartitionSpec as P

ITERS = 8
penalty = 1.0
aug_weight = 1.0
step_size = 0.05
eps = 1e-06

SCEN = ("x", "z", "c")
TILE = 256


def local_steps(a_hbm, state, scale, rhs, mult, x_out, m_out, a_v, at_v, x_v, w_v, sem):
    blocks, rows, width = a_hbm.shape
    own = x_v.shape[1]
    chunks = rows // TILE

    def load(b, r):
        piece = pl.ds(r * TILE, TILE)
        return pltpu.make_async_copy(a_hbm.at[b, piece], a_v.at[b, piece], sem.at[b, r])

    for b in range(blocks):
        for r in range(chunks):
            load(b, r).start()
    for b in range(blocks):
        x_v[b] = state[b, own : 2 * own]
        for r in range(chunks):
            load(b, r).wait()

        @pl.loop(0, chunks)
        def _(r):
            at = pl.ds(pl.multiple_of(r * TILE, TILE), TILE)
            for j in range(width // TILE):
                col = slice(j * TILE, (j + 1) * TILE)
                at_v[b * width + j * TILE : b * width + (j + 1) * TILE, at] = a_v[b, at, col].T

    def residual(j):
        col = slice(j * TILE, (j + 1) * TILE)
        xb = jnp.concatenate([x_v[b] for b in range(blocks)], axis=1).astype(jnp.bfloat16)
        prod = jnp.dot(xb, at_v[:, col], preferred_element_type=jnp.float32)
        return mult[:, col] + aug_weight * (scale[:, col] * prod - rhs[:, col])

    @pl.loop(0, ITERS)
    def _(i):
        for j in range(chunks):
            col = slice(j * TILE, (j + 1) * TILE)
            w_v[:, col] = (scale[:, col] * residual(j)).astype(jnp.bfloat16)
        for b in range(blocks):
            for j in range(width // TILE):
                col = slice(j * TILE, (j + 1) * TILE)
                back = jnp.dot(w_v[...], a_v[b, :, col], preferred_element_type=jnp.float32)
                x = x_v[b, :, col]
                grad = state[b, :own, col] + penalty * x + back
                box = state[b, 2 * own : 2 * own + 1, col]
                x_v[b, :, col] = jnp.clip(x - step_size * grad, -box, box)

    share = rows // blocks
    for j in range(chunks):
        at = j * TILE
        m_out[at // share, :, at % share : at % share + TILE] = residual(j)
    x_out[...] = x_v[...]


def run_local(matrix, state, scale, rhs, mult):
    blocks, rows, width = matrix.shape
    own = scale.shape[0]
    vmem = pl.BlockSpec(memory_space=pltpu.VMEM)
    return pl.pallas_call(
        local_steps,
        out_shape=(
            jax.ShapeDtypeStruct((blocks, own, width), jnp.float32),
            jax.ShapeDtypeStruct((blocks, own, rows // blocks), jnp.float32),
        ),
        in_specs=[pl.BlockSpec(memory_space=pl.ANY)] + [vmem] * 4,
        out_specs=(vmem, vmem),
        scratch_shapes=[
            pltpu.VMEM((blocks, rows, width), jnp.bfloat16),
            pltpu.VMEM((blocks * width, rows), jnp.bfloat16),
            pltpu.VMEM((blocks, own, width), jnp.float32),
            pltpu.VMEM((own, rows), jnp.bfloat16),
            pltpu.SemaphoreType.DMA((blocks, rows // TILE)),
        ],
        compiler_params=pltpu.CompilerParams(vmem_limit_bytes=48 * 1024 * 1024),
        cost_estimate=pl.CostEstimate(
            flops=2 * (2 * ITERS + 1) * own * rows * blocks * width,
            bytes_accessed=2 * blocks * rows * width,
            transcendentals=0,
        ),
        name="local_steps",
    )(matrix, state, scale, rhs, mult)


def shift(value, axis, by):
    n = lax.axis_size(axis)
    return lax.ppermute(value, axis, [(i, (i + by) % n) for i in range(n)])


def ring_sum(value, axis):
    return (value + shift(value, axis, 2)) + (shift(value, axis, 1) + shift(value, axis, 3))


def per_device(cons_matrix, row_scale, rhs, cons_mult, cost, ph_mult, start, consensus, upper, prob):
    blocks = lax.axis_size("y")
    me = lax.axis_index("y")
    rows, width = cons_matrix.shape
    group = start.shape[0]
    own = group // blocks

    n_scen = lax.axis_size(SCEN)
    piece = rows // n_scen
    mine = lax.dynamic_slice_in_dim(cons_matrix, lax.axis_index(SCEN) * piece, piece, 0)
    matrix = lax.all_gather(mine, ("y",) + SCEN).reshape(blocks, rows, width)

    linear = cost + ph_mult - penalty * consensus[None, :]
    box = jnp.broadcast_to(upper[None, None, :], (blocks, 8, width))
    sent = jnp.concatenate(
        [linear.reshape(blocks, own, width), start.reshape(blocks, own, width), box], axis=1
    )
    state = lax.all_to_all(sent, "y", 0, 0, tiled=True)
    cut = lambda a: lax.dynamic_slice_in_dim(a, me * own, own, 0)
    x_own, m_own = run_local(matrix, state, cut(row_scale), cut(rhs), cut(cons_mult))

    back = lax.all_to_all(jnp.concatenate([x_own, m_own], axis=2), "y", 0, 0, tiled=True)
    back = back.reshape(group, -1)
    x, mult_new = back[:, :width], back[:, width:]

    weighted = prob[:, None] * x
    parts = jnp.concatenate(
        [
            jnp.sum(weighted, axis=0),
            jnp.full((8,), jnp.sum(prob)),
            jnp.full((8,), jnp.sum(weighted * x)),
        ]
    )
    parts = parts + lax.ppermute(parts, "c", [(0, 1), (1, 0)])
    parts = ring_sum(ring_sum(parts, "x"), "z")
    total, square = parts[width], parts[width + 8]
    z_new = parts[:width] / total
    primal_block = square - total * jnp.sum(z_new * z_new)
    dual_block = jnp.sum((z_new - consensus) ** 2)
    norms = ring_sum(jnp.concatenate([jnp.full((8,), primal_block), jnp.full((8,), dual_block)]), "y")
    w_new = ph_mult + penalty * (x - z_new[None, :])
    n_vars = blocks * width
    primal_res = jnp.sqrt(norms[0] / (total * n_vars) + eps)
    dual_res = penalty * jnp.sqrt(norms[8] / n_vars + eps)
    return (x, mult_new, z_new, w_new, primal_res, dual_res)


def solution(mesh):
    fine = Mesh(mesh.devices.reshape(4, 4, 2, 4), SCEN + ("y",))
    in_specs = (
        P(None, "y"),
        P(SCEN, None),
        P(SCEN, None),
        P(SCEN, None),
        P(SCEN, "y"),
        P(SCEN, "y"),
        P(SCEN, "y"),
        P("y"),
        P("y"),
        P(SCEN),
    )
    out_specs = (P(SCEN, "y"), P(SCEN, "y"), P("y"), P(SCEN, "y"), P(), P())
    return jax.shard_map(
        per_device, mesh=fine, in_specs=in_specs, out_specs=out_specs, check_vma=False
    )
```

```python
import jax
import jax.numpy as jnp
from jax import lax
from jax.experimental import pallas as pl
from jax.experimental.pallas import tpu as pltpu
from jax.sharding import Mesh
from jax.sharding import PartitionSpec as P

ITERS = 8
penalty = 1.0
aug_weight = 1.0
step_size = 0.05
eps = 1e-06


SCEN = ("x", "z", "c")
ALL = ("x", "z", "c", "y")
RING = 4
TILE = 256


def pairs(move):
    def flat(x, z, c, y):
        return ((x * RING + z) * 2 + c) * RING + y

    spots = [
        (x, z, c, y) for x in range(RING) for z in range(RING) for c in range(2) for y in range(RING)
    ]
    return [(flat(*spot), flat(*move(*spot))) for spot in spots]


def along(step):
    def move(x, z, c, y):
        return ((x + step) % RING, z, c, y) if c == 0 else (x, (z + step) % RING, c, y)

    return pairs(move)


FIRST = pairs(lambda x, z, c, y: (x, z, c, y ^ 1 if c == 0 else 3 - y))
SECOND = pairs(lambda x, z, c, y: (x, z, c, 3 - y if c == 0 else y ^ 1))
OTHER = pairs(lambda x, z, c, y: (x, z, 1 - c, y))
UP, DOWN = along(1), along(-1)


def send(value, perm):
    return lax.ppermute(value, ALL, perm)


def ring_place():
    x, z, c = lax.axis_index("x"), lax.axis_index("z"), lax.axis_index("c")
    return c, jnp.where(c == 0, x, z), jnp.where(c == 0, z, x)


def gather_matrix(matrix):
    c, i, _ = ring_place()
    half = matrix.shape[0] // 2
    quarter = half // RING
    own = lax.dynamic_slice_in_dim(matrix, c * half + i * quarter, quarter, 0)
    one = send(own, FIRST)
    two = send(own, SECOND)
    three = send(one, SECOND)
    mine = []
    for k, block in enumerate((one, two, three)):
        up, down = send(block, UP), send(block, DOWN)
        if k == 0:
            far = [send(up, UP)]
        elif k == 1:
            far = [send(down, DOWN)]
        else:
            far = [send(up[: quarter // 2], UP), send(down[quarter // 2 :], DOWN)]
        mine.append([block, up, down] + far)
    theirs = [[send(piece, OTHER) for piece in block] for block in mine]
    return mine, theirs


def local_steps(place, *refs):
    pieces, refs = refs[:26], refs[26:]
    own_a, scale_h, rhs_h, mult_h, weight_h, state, out, parts = refs[:8]
    a_v, at_v, x_v, w_v, back_v, scale, rhs, mult, weight, sem, row_sem = refs[8:]
    slots, width = a_v.shape[1], a_v.shape[3]
    n_piece = a_v.shape[0]
    rows = n_piece * TILE
    own = x_v.shape[1]
    first = pl.multiple_of(place[12], 8)

    def offset(p):
        return pl.multiple_of(place[p], TILE)

    waits = []
    for p in range(n_piece):
        at = pl.ds(p * TILE, TILE)
        for k, (src, dst) in enumerate(((scale_h, scale), (rhs_h, rhs), (mult_h, mult))):
            copy = pltpu.make_async_copy(
                src.at[pl.ds(first, own), pl.ds(offset(p), TILE)], dst.at[:, at], row_sem.at[p * 3 + k]
            )
            copy.start()
            waits.append(copy)
    copy = pltpu.make_async_copy(weight_h.at[pl.ds(first, own)], weight, row_sem.at[3 * n_piece])
    copy.start()
    waits.append(copy)

    per_half = n_piece // 2
    for p in range(n_piece):
        pltpu.make_async_copy(own_a.at[pl.ds(offset(p), TILE)], a_v.at[p, 0], sem.at[p]).start()
        side, q = divmod(p, per_half)
        for k in range(3):
            slot = 1 + (k if side == 0 else (1, 0, 2)[k])
            base = side * 13 + k * 4
            if q == 3 and k == 2:
                for h in range(2):
                    rows_h = pl.ds(h * TILE // 2, TILE // 2)
                    pltpu.make_async_copy(pieces[base + 3 + h], a_v.at[p, slot, rows_h], sem.at[p]).start()
            else:
                pltpu.make_async_copy(pieces[base + q], a_v.at[p, slot], sem.at[p]).start()

    for b in range(slots):
        x_v[b] = state[place[8 + b], own : 2 * own]
    for copy in waits:
        copy.wait()

    def turned(p):
        pltpu.make_async_copy(a_v.at[p], a_v.at[p], sem.at[p]).wait()
        at = pl.ds(pl.multiple_of(p * TILE, TILE), TILE)
        for b in range(slots):
            for j in range(width // TILE):
                var = b * width + j * TILE
                at_v[var : var + TILE, at] = a_v[p, b, :, j * TILE : (j + 1) * TILE].T

    def current():
        return jnp.concatenate([x_v[b] for b in range(slots)], axis=1).astype(jnp.bfloat16)

    def residual(p, xb):
        at = pl.ds(pl.multiple_of(p * TILE, TILE), TILE)
        prod = jnp.dot(xb, at_v[:, at], preferred_element_type=jnp.float32)
        return mult[:, at] + aug_weight * (scale[:, at] * prod - rhs[:, at])

    def weigh(p, xb):
        at = pl.ds(pl.multiple_of(p * TILE, TILE), TILE)
        w_v[:, at] = (scale[:, at] * residual(p, xb)).astype(jnp.bfloat16)

    def add_back(p):
        at = pl.ds(pl.multiple_of(p * TILE, TILE), TILE)
        for b in range(slots):
            for j in range(width // TILE):
                col = slice(j * TILE, (j + 1) * TILE)
                back_v[b, :, col] += jnp.dot(
                    w_v[:, at], a_v[p, b, :, col], preferred_element_type=jnp.float32
                )

    def move(b, col, back):
        block = place[8 + b]
        x = x_v[b, :, col]
        grad = state[block, :own, col] + penalty * x + back
        box = state[block, 2 * own : 2 * own + 1, col]
        x_v[b, :, col] = jnp.clip(x - step_size * grad, -box, box)

    back_v[...] = jnp.zeros_like(back_v)
    turned(0)
    weigh(0, current())

    @pl.loop(1, n_piece)
    def _(p):
        turned(p)
        add_back(p - 1)
        weigh(p, current())

    add_back(n_piece - 1)
    for b in range(slots):
        for j in range(width // TILE):
            col = slice(j * TILE, (j + 1) * TILE)
            move(b, col, back_v[b, :, col])

    @pl.loop(1, ITERS)
    def _(i):
        xb = current()
        for p in range(n_piece):
            weigh(p, xb)
        w = w_v[...]
        for b in range(slots):
            for j in range(width // TILE):
                col = slice(j * TILE, (j + 1) * TILE)
                tall = a_v[:, b, :, col].reshape(rows, TILE)
                move(b, col, jnp.dot(w, tall, preferred_element_type=jnp.float32))

    share = rows // slots
    xb = current()
    for p in range(n_piece):
        at = place[p]
        inside = pl.ds(pl.multiple_of(width + lax.rem(at, share), TILE), TILE)
        out[lax.div(at, share), :, inside] = residual(p, xb)
    square = jnp.zeros((1, 1), jnp.float32)
    for b in range(slots):
        block = place[8 + b]
        x = x_v[b]
        out[block, :, :width] = x
        weighted = weight[:, :1] * x
        parts[pl.ds(block, 1), :] = jnp.sum(weighted, axis=0, keepdims=True)
        square += jnp.sum(weighted * x, keepdims=True)
    total = jnp.sum(weight[:, :1], axis=0, keepdims=True)
    parts[4:5, :] = jnp.broadcast_to(total, (1, width))
    parts[5:6, :] = jnp.broadcast_to(square, (1, width))
    parts[6:8, :] = jnp.zeros((2, width), jnp.float32)


def run_local(place, mine, theirs, matrix, scale, rhs, mult, weight, state):
    rows, width = matrix.shape
    blocks = state.shape[0]
    own = scale.shape[0] // blocks
    n_piece = rows // TILE
    pieces = [piece for block in mine + theirs for piece in block]
    vmem = pl.BlockSpec(memory_space=pltpu.VMEM)
    hbm = pl.BlockSpec(memory_space=pltpu.HBM)
    smem = pl.BlockSpec(memory_space=pltpu.SMEM)
    per_row = pltpu.VMEM((own, rows), jnp.float32)
    return pl.pallas_call(
        local_steps,
        out_shape=(
            jax.ShapeDtypeStruct((blocks, own, width + rows // blocks), jnp.float32),
            jax.ShapeDtypeStruct((8, width), jnp.float32),
        ),
        in_specs=[smem] + [hbm] * (len(pieces) + 5) + [vmem],
        out_specs=(vmem, vmem),
        scratch_shapes=[
            pltpu.VMEM((n_piece, blocks, TILE, width), jnp.bfloat16),
            pltpu.VMEM((blocks * width, rows), jnp.bfloat16),
            pltpu.VMEM((blocks, own, width), jnp.float32),
            pltpu.VMEM((own, rows), jnp.bfloat16),
            pltpu.VMEM((blocks, own, width), jnp.float32),
            per_row,
            per_row,
            per_row,
            pltpu.VMEM((own, 128), jnp.float32),
            pltpu.SemaphoreType.DMA((n_piece,)),
            pltpu.SemaphoreType.DMA((3 * n_piece + 1,)),
        ],
        compiler_params=pltpu.CompilerParams(vmem_limit_bytes=44 * 1024 * 1024),
        cost_estimate=pl.CostEstimate(
            flops=2 * (2 * ITERS + 1) * own * rows * blocks * width,
            bytes_accessed=2 * blocks * rows * width,
            transcendentals=0,
        ),
        name="local_steps",
    )(place, *pieces, matrix, scale, rhs, mult, weight, state)


def shift(value, axis, by):
    n = lax.axis_size(axis)
    return lax.ppermute(value, axis, [(i, (i + by) % n) for i in range(n)])


def ring_sum(value, axis):
    return (value + shift(value, axis, 2)) + (shift(value, axis, 1) + shift(value, axis, 3))


def per_device(cons_matrix, row_scale, rhs, cons_mult, cost, ph_mult, start, consensus, upper, prob):
    blocks = lax.axis_size("y")
    me = lax.axis_index("y")
    rows, width = cons_matrix.shape
    group = start.shape[0]
    own = group // blocks

    mine, theirs = gather_matrix(cons_matrix)

    linear = cost + ph_mult - penalty * consensus[None, :]
    flat = jnp.concatenate([upper[None], consensus[None], jnp.zeros((6, width), jnp.float32)])
    box = jnp.broadcast_to(flat[None], (blocks, 8, width))
    sent = jnp.concatenate(
        [linear.reshape(blocks, own, width), start.reshape(blocks, own, width), box], axis=1
    )
    state = lax.all_to_all(sent, "y", 0, 0, tiled=True)

    c, i, j = ring_place()
    half = rows // 2
    turn = jnp.array([0, 3, 1, 2], jnp.int32)
    near, far = me ^ 1, 3 - me
    place = jnp.concatenate(
        [
            c * half + (i + turn) % RING * TILE,
            (1 - c) * half + (j + turn) % RING * TILE,
            jnp.stack([me, jnp.where(c == 0, near, far), jnp.where(c == 0, far, near), me ^ 2]),
            jnp.stack([me * own]),
        ]
    ).astype(jnp.int32)
    weight = jnp.broadcast_to(prob[:, None], (group, 128))
    result, parts = run_local(
        place, mine, theirs, cons_matrix, row_scale, rhs, cons_mult, weight, state
    )

    back = lax.all_to_all(result, "y", 0, 0, tiled=True).reshape(group, -1)
    x, mult_new = back[:, :width], back[:, width:]

    parts = parts + lax.ppermute(parts, "c", [(0, 1), (1, 0)])
    parts = ring_sum(ring_sum(ring_sum(parts, "x"), "z"), "y")
    total, square = parts[blocks, 0], parts[blocks + 1, 0]
    z_all = parts[:blocks] / total
    z_new = lax.dynamic_slice_in_dim(z_all, me, 1, 0)
    old = state[:, 2 * own + 1]
    n_vars = blocks * width
    primal_sum = square - total * jnp.sum(z_all * z_all)
    primal_res = jnp.sqrt(primal_sum / (total * n_vars) + eps)
    dual_res = penalty * jnp.sqrt(jnp.sum((z_all - old) ** 2) / n_vars + eps)
    w_new = ph_mult + penalty * (x - z_new)
    return (x, mult_new, z_new[0], w_new, primal_res, dual_res)


def solution(mesh):
    fine = Mesh(mesh.devices.reshape(RING, RING, 2, RING), ALL)
    in_specs = (
        P(None, "y"),
        P(SCEN, None),
        P(SCEN, None),
        P(SCEN, None),
        P(SCEN, "y"),
        P(SCEN, "y"),
        P(SCEN, "y"),
        P("y"),
        P("y"),
        P(SCEN),
    )
    out_specs = (P(SCEN, "y"), P(SCEN, "y"), P("y"), P(SCEN, "y"), P(), P())
    return jax.shard_map(
        per_device, mesh=fine, in_specs=in_specs, out_specs=out_specs, check_vma=False
    )
```

```python
import jax
import jax.numpy as jnp
from jax import lax
from jax.experimental import pallas as pl
from jax.experimental.pallas import tpu as pltpu
from jax.sharding import Mesh
from jax.sharding import PartitionSpec as P


ITERS = 8
penalty = 1.0
aug_weight = 1.0
step_size = 0.05
eps = 1e-06


SCEN = ("x", "z", "c")
ALL = ("x", "z", "c", "y")
RING = 4
TILE = 256


def pairs(move):
    def flat(x, z, c, y):
        return ((x * RING + z) * 2 + c) * RING + y

    spots = [
        (x, z, c, y) for x in range(RING) for z in range(RING) for c in range(2) for y in range(RING)
    ]
    return [(flat(*spot), flat(*move(*spot))) for spot in spots]


def along(step):
    def move(x, z, c, y):
        return ((x + step) % RING, z, c, y) if c == 0 else (x, (z + step) % RING, c, y)

    return pairs(move)


FIRST = pairs(lambda x, z, c, y: (x, z, c, y ^ 1 if c == 0 else 3 - y))
SECOND = pairs(lambda x, z, c, y: (x, z, c, 3 - y if c == 0 else y ^ 1))
OTHER = pairs(lambda x, z, c, y: (x, z, 1 - c, y))
UP, DOWN = along(1), along(-1)


def send(value, perm):
    return lax.ppermute(value, ALL, perm)


def ring_place():
    x, z, c = lax.axis_index("x"), lax.axis_index("z"), lax.axis_index("c")
    return c, jnp.where(c == 0, x, z), jnp.where(c == 0, z, x)


def gather_matrix(matrix, far):
    c, i, _ = ring_place()
    half = matrix.shape[0] // 2
    quarter = half // RING
    own = lax.dynamic_slice_in_dim(matrix, c * half + i * quarter, quarter, 0)
    one = send(own, FIRST)
    three = send(one, SECOND)
    two = send(own, SECOND)
    up1, down1 = send(one, UP), send(one, DOWN)
    up3, down3 = send(three, UP), send(three, DOWN)
    up2, down2 = send(two, UP), send(two, DOWN)
    far1 = send(up1, UP)
    far2 = send(far, SECOND)
    far3 = send(down3, DOWN)
    mine = [[one, up1, down1, far1], [two, up2, down2, far2], [three, up3, down3, far3]]
    theirs = [[send(piece, OTHER) for piece in block] for block in mine]
    return mine, theirs


def prepare(place, cost_h, ph_h, start_h, consensus, upper, matrix, sent, far, cost, ph_mult, start, sem):
    loads = ((cost_h, cost), (ph_h, ph_mult), (start_h, start))
    loads += ((matrix.at[pl.ds(pl.multiple_of(place[3], TILE), TILE)], far),)
    copies = [pltpu.make_async_copy(src, dst, sem.at[k]) for k, (src, dst) in enumerate(loads)]
    for copy in copies:
        copy.start()
    blocks, rows, width = sent.shape
    own = (rows - 8) // 2
    flat = jnp.concatenate([upper[...], consensus[...], jnp.zeros((6, width), jnp.float32)], axis=0)
    for b in range(blocks):
        sent[b, 2 * own :] = flat
    for copy in copies[:3]:
        copy.wait()
    for b in range(blocks):
        at = slice(b * own, (b + 1) * own)
        sent[b, :own] = cost[at] + ph_mult[at] - penalty * consensus[...]
        sent[b, own : 2 * own] = start[at]
    copies[3].wait()


def run_prepare(place, cost, ph_mult, start, consensus, upper, matrix, blocks):
    group, width = start.shape
    vmem = pl.BlockSpec(memory_space=pltpu.VMEM)
    hbm = pl.BlockSpec(memory_space=pltpu.HBM)
    held = pltpu.VMEM((group, width), jnp.float32)
    return pl.pallas_call(
        prepare,
        out_shape=(
            jax.ShapeDtypeStruct((blocks, 2 * group // blocks + 8, width), jnp.float32),
            jax.ShapeDtypeStruct((TILE, width), jnp.bfloat16),
        ),
        in_specs=[pl.BlockSpec(memory_space=pltpu.SMEM)] + [hbm] * 3 + [vmem] * 2 + [hbm],
        out_specs=(vmem, vmem),
        scratch_shapes=[held, held, held, pltpu.SemaphoreType.DMA((4,))],
        compiler_params=pltpu.CompilerParams(vmem_limit_bytes=8 * 1024 * 1024),
        cost_estimate=pl.CostEstimate(
            flops=4000000, bytes_accessed=5 * group * width * 4, transcendentals=0
        ),
        name="prepare",
    )(place, cost, ph_mult, start, consensus[None], upper[None], matrix)


def finish(place, p0, p1, p2, p3, back, ph_mult, old, x, mult, z, w, primal, dual):
    blocks, own, _ = back.shape
    width = x.shape[1]
    n_vars = blocks * width
    parts = (p0[...] + p2[...]) + (p1[...] + p3[...])
    total, square = parts[blocks : blocks + 1, :1], parts[blocks + 1 : blocks + 2, :1]
    z_all = parts[:blocks] / total
    primal_sum = square - total * jnp.sum(z_all * z_all, keepdims=True)
    primal[...] = jnp.sqrt(primal_sum / (total * n_vars) + eps)
    gap = z_all - old[...]
    dual[...] = penalty * jnp.sqrt(jnp.sum(gap * gap, keepdims=True) / n_vars + eps)
    mine = lax.broadcasted_iota(jnp.int32, (blocks, 1), 0) == place[8]
    z_own = jnp.sum(jnp.where(mine, z_all, 0.0), axis=0, keepdims=True)
    z[...] = z_own
    for b in range(blocks):
        at = slice(b * own, (b + 1) * own)
        solved = back[b, :, :width]
        x[at] = solved
        mult[at] = back[b, :, width:]
        w[at] = ph_mult[at] + penalty * (solved - z_own)


def run_finish(place, shares, back, ph_mult, old):
    _, _, both = back.shape
    group, width = ph_mult.shape
    vmem = pl.BlockSpec(memory_space=pltpu.VMEM)
    shapes = ((group, width), (group, both - width), (1, width), (group, width), (1, 1), (1, 1))
    return pl.pallas_call(
        finish,
        out_shape=tuple(jax.ShapeDtypeStruct(shape, jnp.float32) for shape in shapes),
        in_specs=[pl.BlockSpec(memory_space=pltpu.SMEM)] + [vmem] * 7,
        out_specs=(vmem,) * 6,
        compiler_params=pltpu.CompilerParams(vmem_limit_bytes=8 * 1024 * 1024),
        cost_estimate=pl.CostEstimate(
            flops=4000000, bytes_accessed=5 * group * width * 4, transcendentals=0
        ),
        name="finish",
    )(place, *shares, back, ph_mult, old)


def local_steps(place, *refs):
    pieces, refs = refs[:24], refs[24:]
    own_a, scale_h, rhs_h, mult_h, weight_h, state, out, parts = refs[:8]
    a_v, at_v, x_v, w_v, back_v, scale, rhs, mult, weight, sem, row_sem = refs[8:]
    slots, width = a_v.shape[1], a_v.shape[3]
    n_piece = a_v.shape[0]
    rows = n_piece * TILE
    own = x_v.shape[1]
    first = pl.multiple_of(place[12], 8)

    def offset(p):
        return pl.multiple_of(place[p], TILE)

    waits = []
    for p in range(n_piece):
        at = pl.ds(p * TILE, TILE)
        for k, (src, dst) in enumerate(((scale_h, scale), (rhs_h, rhs), (mult_h, mult))):
            copy = pltpu.make_async_copy(
                src.at[pl.ds(first, own), pl.ds(offset(p), TILE)], dst.at[:, at], row_sem.at[p * 3 + k]
            )
            copy.start()
            waits.append(copy)
    copy = pltpu.make_async_copy(weight_h.at[pl.ds(first, own)], weight, row_sem.at[3 * n_piece])
    copy.start()
    waits.append(copy)

    per_half = n_piece // 2
    for p in range(n_piece):
        pltpu.make_async_copy(own_a.at[pl.ds(offset(p), TILE)], a_v.at[p, 0], sem.at[p]).start()
        side, q = divmod(p, per_half)
        for k in range(3):
            slot = 1 + (k if side == 0 else (1, 0, 2)[k])
            piece = pieces[side * 12 + k * 4 + q]
            pltpu.make_async_copy(piece, a_v.at[p, slot], sem.at[p]).start()

    for b in range(slots):
        x_v[b] = state[place[8 + b], own : 2 * own]
    for copy in waits:
        copy.wait()

    def turned(p):
        pltpu.make_async_copy(a_v.at[p], a_v.at[p], sem.at[p]).wait()
        at = pl.ds(pl.multiple_of(p * TILE, TILE), TILE)
        for b in range(slots):
            for j in range(width // TILE):
                var = b * width + j * TILE
                at_v[var : var + TILE, at] = a_v[p, b, :, j * TILE : (j + 1) * TILE].T

    def current():
        return jnp.concatenate([x_v[b] for b in range(slots)], axis=1).astype(jnp.bfloat16)

    def residual(p, xb):
        at = pl.ds(pl.multiple_of(p * TILE, TILE), TILE)
        prod = jnp.dot(xb, at_v[:, at], preferred_element_type=jnp.float32)
        return mult[:, at] + aug_weight * (scale[:, at] * prod - rhs[:, at])

    def weigh(p, xb):
        at = pl.ds(pl.multiple_of(p * TILE, TILE), TILE)
        w_v[:, at] = (scale[:, at] * residual(p, xb)).astype(jnp.bfloat16)

    def add_back(p):
        at = pl.ds(pl.multiple_of(p * TILE, TILE), TILE)
        for b in range(slots):
            for j in range(width // TILE):
                col = slice(j * TILE, (j + 1) * TILE)
                back_v[b, :, col] += jnp.dot(
                    w_v[:, at], a_v[p, b, :, col], preferred_element_type=jnp.float32
                )

    def move(b, col, back):
        block = place[8 + b]
        x = x_v[b, :, col]
        grad = state[block, :own, col] + penalty * x + back
        box = state[block, 2 * own : 2 * own + 1, col]
        x_v[b, :, col] = jnp.clip(x - step_size * grad, -box, box)

    back_v[...] = jnp.zeros_like(back_v)
    turned(0)
    weigh(0, current())

    @pl.loop(1, n_piece)
    def _(p):
        turned(p)
        add_back(p - 1)
        weigh(p, current())

    add_back(n_piece - 1)
    for b in range(slots):
        for j in range(width // TILE):
            col = slice(j * TILE, (j + 1) * TILE)
            move(b, col, back_v[b, :, col])

    @pl.loop(1, ITERS)
    def _(i):
        xb = current()
        for p in range(n_piece):
            weigh(p, xb)
        w = w_v[...]
        for b in range(slots):
            for j in range(width // TILE):
                col = slice(j * TILE, (j + 1) * TILE)
                tall = a_v[:, b, :, col].reshape(rows, TILE)
                move(b, col, jnp.dot(w, tall, preferred_element_type=jnp.float32))

    share = rows // slots
    xb = current()
    for p in range(n_piece):
        at = place[p]
        inside = pl.ds(pl.multiple_of(width + lax.rem(at, share), TILE), TILE)
        out[lax.div(at, share), :, inside] = residual(p, xb)
    square = jnp.zeros((1, 1), jnp.float32)
    for b in range(slots):
        block = place[8 + b]
        x = x_v[b]
        out[block, :, :width] = x
        weighted = weight[:, :1] * x
        parts[pl.ds(block, 1), :] = jnp.sum(weighted, axis=0, keepdims=True)
        square += jnp.sum(weighted * x, keepdims=True)
    total = jnp.sum(weight[:, :1], axis=0, keepdims=True)
    parts[4:5, :] = jnp.broadcast_to(total, (1, width))
    parts[5:6, :] = jnp.broadcast_to(square, (1, width))
    parts[6:8, :] = jnp.zeros((2, width), jnp.float32)


def run_local(place, mine, theirs, matrix, scale, rhs, mult, weight, state):
    rows, width = matrix.shape
    blocks = state.shape[0]
    own = scale.shape[0] // blocks
    n_piece = rows // TILE
    pieces = [piece for block in mine + theirs for piece in block]
    vmem = pl.BlockSpec(memory_space=pltpu.VMEM)
    hbm = pl.BlockSpec(memory_space=pltpu.HBM)
    smem = pl.BlockSpec(memory_space=pltpu.SMEM)
    per_row = pltpu.VMEM((own, rows), jnp.float32)
    return pl.pallas_call(
        local_steps,
        out_shape=(
            jax.ShapeDtypeStruct((blocks, own, width + rows // blocks), jnp.float32),
            jax.ShapeDtypeStruct((8, width), jnp.float32),
        ),
        in_specs=[smem] + [hbm] * (len(pieces) + 5) + [vmem],
        out_specs=(vmem, vmem),
        scratch_shapes=[
            pltpu.VMEM((n_piece, blocks, TILE, width), jnp.bfloat16),
            pltpu.VMEM((blocks * width, rows), jnp.bfloat16),
            pltpu.VMEM((blocks, own, width), jnp.float32),
            pltpu.VMEM((own, rows), jnp.bfloat16),
            pltpu.VMEM((blocks, own, width), jnp.float32),
            per_row,
            per_row,
            per_row,
            pltpu.VMEM((own, 128), jnp.float32),
            pltpu.SemaphoreType.DMA((n_piece,)),
            pltpu.SemaphoreType.DMA((3 * n_piece + 1,)),
        ],
        compiler_params=pltpu.CompilerParams(vmem_limit_bytes=44 * 1024 * 1024),
        cost_estimate=pl.CostEstimate(
            flops=2 * (2 * ITERS + 1) * own * rows * blocks * width,
            bytes_accessed=2 * blocks * rows * width,
            transcendentals=0,
        ),
        name="local_steps",
    )(place, *pieces, matrix, scale, rhs, mult, weight, state)


def shift(value, axis, by):
    n = lax.axis_size(axis)
    return lax.ppermute(value, axis, [(i, (i + by) % n) for i in range(n)])


def ring_sum(value, axis):
    return (value + shift(value, axis, 2)) + (shift(value, axis, 1) + shift(value, axis, 3))


def per_device(cons_matrix, row_scale, rhs, cons_mult, cost, ph_mult, start, consensus, upper, prob):
    blocks = lax.axis_size("y")
    me = lax.axis_index("y")
    rows, _ = cons_matrix.shape
    group = start.shape[0]
    own = group // blocks

    c, i, j = ring_place()
    half = rows // 2
    turn = jnp.array([0, 3, 1, 2], jnp.int32)
    near, far = me ^ 1, 3 - me
    place = jnp.concatenate(
        [
            c * half + (i + turn) % RING * TILE,
            (1 - c) * half + (j + turn) % RING * TILE,
            jnp.stack([me, jnp.where(c == 0, near, far), jnp.where(c == 0, far, near), me ^ 2]),
            jnp.stack([me * own]),
        ]
    ).astype(jnp.int32)
    sent, far = run_prepare(place, cost, ph_mult, start, consensus, upper, cons_matrix, blocks)
    mine, theirs = gather_matrix(cons_matrix, far)
    state = lax.all_to_all(sent, "y", 0, 0, tiled=True)

    weight = jnp.broadcast_to(prob[:, None], (group, 128))
    result, parts = run_local(
        place, mine, theirs, cons_matrix, row_scale, rhs, cons_mult, weight, state
    )

    back = lax.all_to_all(result, "y", 0, 0, tiled=True)
    parts = parts + send(parts, OTHER)
    parts = ring_sum(ring_sum(parts, "x"), "z")
    shares = (parts, shift(parts, "y", 1), shift(parts, "y", 2), shift(parts, "y", 3))
    x, mult_new, z_new, w_new, primal_res, dual_res = run_finish(
        place, shares, back, ph_mult, state[:, 2 * own + 1]
    )
    return (x, mult_new, z_new[0], w_new, primal_res[0, 0], dual_res[0, 0])


def solution(mesh):
    fine = Mesh(mesh.devices.reshape(RING, RING, 2, RING), ALL)
    in_specs = (
        P(None, "y"),
        P(SCEN, None),
        P(SCEN, None),
        P(SCEN, None),
        P(SCEN, "y"),
        P(SCEN, "y"),
        P(SCEN, "y"),
        P("y"),
        P("y"),
        P(SCEN),
    )
    out_specs = (P(SCEN, "y"), P(SCEN, "y"), P("y"), P(SCEN, "y"), P(), P())
    return jax.shard_map(per_device, mesh=fine, in_specs=in_specs, out_specs=out_specs, check_vma=False)
```

```python
import jax
import jax.numpy as jnp
from jax import lax
from jax.experimental import pallas as pl
from jax.experimental.pallas import tpu as pltpu
from jax.sharding import Mesh
from jax.sharding import PartitionSpec as P


ITERS = 8
penalty = 1.0
aug_weight = 1.0
step_size = 0.05
eps = 1e-06


SCEN = ("x", "z", "c")
ALL = ("x", "z", "c", "y")
RING = 4
TILE = 256


def pairs(move):
    def flat(x, z, c, y):
        return ((x * RING + z) * 2 + c) * RING + y

    spots = [
        (x, z, c, y) for x in range(RING) for z in range(RING) for c in range(2) for y in range(RING)
    ]
    return [(flat(*spot), flat(*move(*spot))) for spot in spots]


def along(step):
    def move(x, z, c, y):
        return ((x + step) % RING, z, c, y) if c == 0 else (x, (z + step) % RING, c, y)

    return pairs(move)


FIRST = pairs(lambda x, z, c, y: (x, z, c, y ^ 1 if c == 0 else 3 - y))
SECOND = pairs(lambda x, z, c, y: (x, z, c, 3 - y if c == 0 else y ^ 1))
OTHER = pairs(lambda x, z, c, y: (x, z, 1 - c, y))
UP, DOWN = along(1), along(-1)


def send(value, perm):
    return lax.ppermute(value, ALL, perm)


def ring_place():
    x, z, c = lax.axis_index("x"), lax.axis_index("z"), lax.axis_index("c")
    return c, jnp.where(c == 0, x, z), jnp.where(c == 0, z, x)


def gather_matrix(matrix, far):
    c, i, _ = ring_place()
    half = matrix.shape[0] // 2
    quarter = half // RING
    own = lax.dynamic_slice_in_dim(matrix, c * half + i * quarter, quarter, 0)
    one = send(own, FIRST)
    three = send(one, SECOND)
    two = send(own, SECOND)
    up1, down1 = send(one, UP), send(one, DOWN)
    up3, down3 = send(three, UP), send(three, DOWN)
    up2, down2 = send(two, UP), send(two, DOWN)
    far1 = send(far, FIRST)
    far2 = send(far, SECOND)
    far3 = send(down3, DOWN)
    mine = [[one, up1, down1, far1], [two, up2, down2, far2], [three, up3, down3, far3]]
    theirs = [[send(piece, OTHER) for piece in block] for block in mine]
    return mine, theirs


def prepare(place, cost_h, ph_h, start_h, consensus, upper, matrix, kept, one, opposite, two, far, *scratch):
    cost, ph_mult, start, sem = scratch
    loads = ((cost_h, cost), (ph_h, ph_mult), (start_h, start))
    loads += ((matrix.at[pl.ds(pl.multiple_of(place[3], TILE), TILE)], far),)
    copies = [pltpu.make_async_copy(src, dst, sem.at[k]) for k, (src, dst) in enumerate(loads)]
    for copy in copies:
        copy.start()
    rows, width = kept.shape
    own = (rows - 8) // 2
    flat = jnp.concatenate([upper[...], consensus[...], jnp.zeros((6, width), jnp.float32)], axis=0)
    for sent in (kept, one, two, opposite):
        sent[2 * own :] = flat
    for copy in copies[:3]:
        copy.wait()
    for slot, sent in enumerate((kept, one, two, opposite)):
        at = pl.ds(pl.multiple_of(place[8 + slot] * own, own), own)
        sent[:own] = cost[at] + ph_mult[at] - penalty * consensus[...]
        sent[own : 2 * own] = start[at]
    copies[3].wait()


def run_prepare(place, cost, ph_mult, start, consensus, upper, matrix, blocks):
    group, width = start.shape
    vmem = pl.BlockSpec(memory_space=pltpu.VMEM)
    hbm = pl.BlockSpec(memory_space=pltpu.HBM)
    held = pltpu.VMEM((group, width), jnp.float32)
    state = jax.ShapeDtypeStruct((2 * group // blocks + 8, width), jnp.float32)
    return pl.pallas_call(
        prepare,
        out_shape=(state, state, state, state, jax.ShapeDtypeStruct((TILE, width), jnp.bfloat16)),
        in_specs=[pl.BlockSpec(memory_space=pltpu.SMEM)] + [hbm] * 3 + [vmem] * 2 + [hbm],
        out_specs=(vmem,) * 5,
        scratch_shapes=[held, held, held, pltpu.SemaphoreType.DMA((4,))],
        compiler_params=pltpu.CompilerParams(vmem_limit_bytes=60 * 1024 * 1024),
        cost_estimate=pl.CostEstimate(
            flops=4000000, bytes_accessed=5 * group * width * 4, transcendentals=0
        ),
        name="prepare",
    )(place, cost, ph_mult, start, consensus[None], upper[None], matrix)


def finish(place, p0, p1, p2, p3, back, ph_mult, old, x, mult, z, w, primal, dual):
    blocks, own, _ = back.shape
    width = x.shape[1]
    n_vars = blocks * width
    parts = (p0[...] + p2[...]) + (p1[...] + p3[...])
    total, square = parts[blocks : blocks + 1, :1], parts[blocks + 1 : blocks + 2, :1]
    z_all = parts[:blocks] / total
    primal_sum = square - total * jnp.sum(z_all * z_all, keepdims=True)
    primal[...] = jnp.sqrt(primal_sum / (total * n_vars) + eps)
    gap = z_all - old[...]
    dual[...] = penalty * jnp.sqrt(jnp.sum(gap * gap, keepdims=True) / n_vars + eps)
    mine = lax.broadcasted_iota(jnp.int32, (blocks, 1), 0) == place[8]
    z_own = jnp.sum(jnp.where(mine, z_all, 0.0), axis=0, keepdims=True)
    z[...] = z_own
    for b in range(blocks):
        at = slice(b * own, (b + 1) * own)
        solved = back[b, :, :width]
        x[at] = solved
        mult[at] = back[b, :, width:]
        w[at] = ph_mult[at] + penalty * (solved - z_own)


def run_finish(place, shares, back, ph_mult, old):
    _, _, both = back.shape
    group, width = ph_mult.shape
    vmem = pl.BlockSpec(memory_space=pltpu.VMEM)
    shapes = ((group, width), (group, both - width), (1, width), (group, width), (1, 1), (1, 1))
    return pl.pallas_call(
        finish,
        out_shape=tuple(jax.ShapeDtypeStruct(shape, jnp.float32) for shape in shapes),
        in_specs=[pl.BlockSpec(memory_space=pltpu.SMEM)] + [vmem] * 7,
        out_specs=(vmem,) * 6,
        compiler_params=pltpu.CompilerParams(vmem_limit_bytes=8 * 1024 * 1024),
        cost_estimate=pl.CostEstimate(
            flops=4000000, bytes_accessed=5 * group * width * 4, transcendentals=0
        ),
        name="finish",
    )(place, *shares, back, ph_mult, old)


def local_steps(place, *refs):
    pieces, refs = refs[:24], refs[24:]
    own_a, scale_h, rhs_h, mult_h, weight_h = refs[:5]
    state, (out, parts, old) = refs[5:9], refs[9:12]
    a_v, at_v, x_v, w_v, back_v, scale, rhs, mult, weight, sem, row_sem = refs[12:]
    slots, width = a_v.shape[1], a_v.shape[3]
    n_piece = a_v.shape[0]
    rows = n_piece * TILE
    own = x_v.shape[1]
    first = pl.multiple_of(place[12], 8)

    def offset(p):
        return pl.multiple_of(place[p], TILE)

    waits = []
    for p in range(n_piece):
        at = pl.ds(p * TILE, TILE)
        for k, (src, dst) in enumerate(((scale_h, scale), (rhs_h, rhs), (mult_h, mult))):
            copy = pltpu.make_async_copy(
                src.at[pl.ds(first, own), pl.ds(offset(p), TILE)], dst.at[:, at], row_sem.at[p * 3 + k]
            )
            copy.start()
            waits.append(copy)
    copy = pltpu.make_async_copy(weight_h.at[pl.ds(first, own)], weight, row_sem.at[3 * n_piece])
    copy.start()
    waits.append(copy)

    per_half = n_piece // 2
    for p in range(n_piece):
        pltpu.make_async_copy(own_a.at[pl.ds(offset(p), TILE)], a_v.at[p, 0], sem.at[p]).start()
        side, q = divmod(p, per_half)
        for k in range(3):
            slot = 1 + (k if side == 0 else (1, 0, 2)[k])
            piece = pieces[side * 12 + k * 4 + q]
            pltpu.make_async_copy(piece, a_v.at[p, slot], sem.at[p]).start()

    for b in range(slots):
        x_v[b] = state[b][own : 2 * own]
        old[pl.ds(place[8 + b], 1)] = state[b][2 * own + 1 : 2 * own + 2]
    for copy in waits:
        copy.wait()

    def turned(p):
        pltpu.make_async_copy(a_v.at[p], a_v.at[p], sem.at[p]).wait()
        at = pl.ds(pl.multiple_of(p * TILE, TILE), TILE)
        for b in range(slots):
            for j in range(width // TILE):
                var = b * width + j * TILE
                at_v[var : var + TILE, at] = a_v[p, b, :, j * TILE : (j + 1) * TILE].T

    def current():
        return jnp.concatenate([x_v[b] for b in range(slots)], axis=1).astype(jnp.bfloat16)

    def residual(p, xb):
        at = pl.ds(pl.multiple_of(p * TILE, TILE), TILE)
        prod = jnp.dot(xb, at_v[:, at], preferred_element_type=jnp.float32)
        return mult[:, at] + aug_weight * (scale[:, at] * prod - rhs[:, at])

    def weigh(p, xb):
        at = pl.ds(pl.multiple_of(p * TILE, TILE), TILE)
        w_v[:, at] = (scale[:, at] * residual(p, xb)).astype(jnp.bfloat16)

    def add_back(p):
        at = pl.ds(pl.multiple_of(p * TILE, TILE), TILE)
        for b in range(slots):
            for j in range(width // TILE):
                col = slice(j * TILE, (j + 1) * TILE)
                back_v[b, :, col] += jnp.dot(
                    w_v[:, at], a_v[p, b, :, col], preferred_element_type=jnp.float32
                )

    def move(b, col, back):
        x = x_v[b, :, col]
        grad = state[b][:own, col] + penalty * x + back
        box = state[b][2 * own : 2 * own + 1, col]
        x_v[b, :, col] = jnp.clip(x - step_size * grad, -box, box)

    back_v[...] = jnp.zeros_like(back_v)
    turned(0)
    weigh(0, current())

    @pl.loop(1, n_piece)
    def _(p):
        turned(p)
        add_back(p - 1)
        weigh(p, current())

    add_back(n_piece - 1)
    for b in range(slots):
        for j in range(width // TILE):
            col = slice(j * TILE, (j + 1) * TILE)
            move(b, col, back_v[b, :, col])

    @pl.loop(1, ITERS)
    def _(i):
        xb = current()
        for p in range(n_piece):
            weigh(p, xb)
        w = w_v[...]
        for b in range(slots):
            for j in range(width // TILE):
                col = slice(j * TILE, (j + 1) * TILE)
                tall = a_v[:, b, :, col].reshape(rows, TILE)
                move(b, col, jnp.dot(w, tall, preferred_element_type=jnp.float32))

    share = rows // slots
    xb = current()
    for p in range(n_piece):
        at = place[p]
        inside = pl.ds(pl.multiple_of(width + lax.rem(at, share), TILE), TILE)
        out[lax.div(at, share), :, inside] = residual(p, xb)
    square = jnp.zeros((1, 1), jnp.float32)
    for b in range(slots):
        block = place[8 + b]
        x = x_v[b]
        out[block, :, :width] = x
        weighted = weight[:, :1] * x
        parts[pl.ds(block, 1), :] = jnp.sum(weighted, axis=0, keepdims=True)
        square += jnp.sum(weighted * x, keepdims=True)
    total = jnp.sum(weight[:, :1], axis=0, keepdims=True)
    parts[4:5, :] = jnp.broadcast_to(total, (1, width))
    parts[5:6, :] = jnp.broadcast_to(square, (1, width))
    parts[6:8, :] = jnp.zeros((2, width), jnp.float32)


def run_local(place, mine, theirs, matrix, scale, rhs, mult, weight, state):
    rows, width = matrix.shape
    blocks = len(state)
    own = scale.shape[0] // blocks
    n_piece = rows // TILE
    pieces = [piece for block in mine + theirs for piece in block]
    vmem = pl.BlockSpec(memory_space=pltpu.VMEM)
    hbm = pl.BlockSpec(memory_space=pltpu.HBM)
    smem = pl.BlockSpec(memory_space=pltpu.SMEM)
    per_row = pltpu.VMEM((own, rows), jnp.float32)
    return pl.pallas_call(
        local_steps,
        out_shape=(
            jax.ShapeDtypeStruct((blocks, own, width + rows // blocks), jnp.float32),
            jax.ShapeDtypeStruct((8, width), jnp.float32),
            jax.ShapeDtypeStruct((blocks, width), jnp.float32),
        ),
        in_specs=[smem] + [hbm] * (len(pieces) + 5) + [vmem] * blocks,
        out_specs=(vmem,) * 3,
        scratch_shapes=[
            pltpu.VMEM((n_piece, blocks, TILE, width), jnp.bfloat16),
            pltpu.VMEM((blocks * width, rows), jnp.bfloat16),
            pltpu.VMEM((blocks, own, width), jnp.float32),
            pltpu.VMEM((own, rows), jnp.bfloat16),
            pltpu.VMEM((blocks, own, width), jnp.float32),
            per_row,
            per_row,
            per_row,
            pltpu.VMEM((own, 128), jnp.float32),
            pltpu.SemaphoreType.DMA((n_piece,)),
            pltpu.SemaphoreType.DMA((3 * n_piece + 1,)),
        ],
        compiler_params=pltpu.CompilerParams(vmem_limit_bytes=37 * 1024 * 1024),
        cost_estimate=pl.CostEstimate(
            flops=2 * (2 * ITERS + 1) * own * rows * blocks * width,
            bytes_accessed=2 * blocks * rows * width,
            transcendentals=0,
        ),
        name="local_steps",
    )(place, *pieces, matrix, scale, rhs, mult, weight, *state)


def shift(value, axis, by):
    n = lax.axis_size(axis)
    return lax.ppermute(value, axis, [(i, (i + by) % n) for i in range(n)])


def ring_sum(value, axis):
    return (value + shift(value, axis, 2)) + (shift(value, axis, 1) + shift(value, axis, 3))


def per_device(cons_matrix, row_scale, rhs, cons_mult, cost, ph_mult, start, consensus, upper, prob):
    blocks = lax.axis_size("y")
    me = lax.axis_index("y")
    rows, _ = cons_matrix.shape
    group = start.shape[0]
    own = group // blocks

    c, i, j = ring_place()
    half = rows // 2
    turn = jnp.array([0, 3, 1, 2], jnp.int32)
    near, far = me ^ 1, 3 - me
    place = jnp.concatenate(
        [
            c * half + (i + turn) % RING * TILE,
            (1 - c) * half + (j + turn) % RING * TILE,
            jnp.stack([me, jnp.where(c == 0, near, far), jnp.where(c == 0, far, near), me ^ 2]),
            jnp.stack([me * own]),
        ]
    ).astype(jnp.int32)
    kept, first, opposite, second, far = run_prepare(
        place, cost, ph_mult, start, consensus, upper, cons_matrix, blocks
    )
    mine, theirs = gather_matrix(cons_matrix, far)
    state = (kept, send(first, FIRST), send(second, SECOND), send(send(opposite, FIRST), SECOND))

    weight = jnp.broadcast_to(prob[:, None], (group, 128))
    result, parts, old = run_local(
        place, mine, theirs, cons_matrix, row_scale, rhs, cons_mult, weight, state
    )

    back = lax.all_to_all(result, "y", 0, 0, tiled=True)
    parts = parts + send(parts, OTHER)
    parts = ring_sum(ring_sum(parts, "x"), "z")
    shares = (parts, shift(parts, "y", 1), shift(parts, "y", 2), shift(parts, "y", 3))
    x, mult_new, z_new, w_new, primal_res, dual_res = run_finish(
        place, shares, back, ph_mult, old
    )
    return (x, mult_new, z_new[0], w_new, primal_res[0, 0], dual_res[0, 0])


def solution(mesh):
    fine = Mesh(mesh.devices.reshape(RING, RING, 2, RING), ALL)
    in_specs = (
        P(None, "y"),
        P(SCEN, None),
        P(SCEN, None),
        P(SCEN, None),
        P(SCEN, "y"),
        P(SCEN, "y"),
        P(SCEN, "y"),
        P("y"),
        P("y"),
        P(SCEN),
    )
    out_specs = (P(SCEN, "y"), P(SCEN, "y"), P("y"), P(SCEN, "y"), P(), P())
    return jax.shard_map(per_device, mesh=fine, in_specs=in_specs, out_specs=out_specs, check_vma=False)
```

```python
import jax
import jax.numpy as jnp
from jax import lax
from jax.experimental import pallas as pl
from jax.experimental.pallas import tpu as pltpu
from jax.sharding import Mesh
from jax.sharding import PartitionSpec as P


ITERS = 8
penalty = 1.0
aug_weight = 1.0
step_size = 0.05
eps = 1e-06


SCEN = ("x", "z", "c")
ALL = ("x", "z", "c", "y")
RING = 4
TILE = 256


def pairs(move):
    def flat(x, z, c, y):
        return ((x * RING + z) * 2 + c) * RING + y

    spots = [
        (x, z, c, y) for x in range(RING) for z in range(RING) for c in range(2) for y in range(RING)
    ]
    return [(flat(*spot), flat(*move(*spot))) for spot in spots]


def along(step):
    def move(x, z, c, y):
        return ((x + step) % RING, z, c, y) if c == 0 else (x, (z + step) % RING, c, y)

    return pairs(move)


FIRST = pairs(lambda x, z, c, y: (x, z, c, y ^ 1 if c == 0 else 3 - y))
SECOND = pairs(lambda x, z, c, y: (x, z, c, 3 - y if c == 0 else y ^ 1))
OTHER = pairs(lambda x, z, c, y: (x, z, 1 - c, y))
UP, DOWN = along(1), along(-1)


def send(value, perm):
    return lax.ppermute(value, ALL, perm)


def ring_place():
    x, z, c = lax.axis_index("x"), lax.axis_index("z"), lax.axis_index("c")
    return c, jnp.where(c == 0, x, z), jnp.where(c == 0, z, x)


def gather_matrix(matrix, far):
    c, i, _ = ring_place()
    half = matrix.shape[0] // 2
    quarter = half // RING
    own = lax.dynamic_slice_in_dim(matrix, c * half + i * quarter, quarter, 0)
    one = send(own, FIRST)
    three = send(one, SECOND)
    two = send(own, SECOND)
    up1, down1 = send(one, UP), send(one, DOWN)
    up3, down3 = send(three, UP), send(three, DOWN)
    up2, down2 = send(two, UP), send(two, DOWN)
    far1 = send(far, FIRST)
    far2 = send(far, SECOND)
    far3 = send(down3, DOWN)
    mine = [[one, up1, down1, far1], [two, up2, down2, far2], [three, up3, down3, far3]]
    theirs = [[send(piece, OTHER) for piece in block] for block in mine]
    return mine, theirs


def prepare(place, cost_h, ph_h, start_h, consensus, upper, matrix, kept, one, opposite, two, far, *scratch):
    cost, ph_mult, start, sem = scratch
    loads = ((cost_h, cost), (ph_h, ph_mult), (start_h, start))
    loads += ((matrix.at[pl.ds(pl.multiple_of(place[3], TILE), TILE)], far),)
    copies = [pltpu.make_async_copy(src, dst, sem.at[k]) for k, (src, dst) in enumerate(loads)]
    for copy in copies:
        copy.start()
    rows, width = kept.shape
    own = (rows - 8) // 2
    flat = jnp.concatenate([upper[...], consensus[...], jnp.zeros((6, width), jnp.float32)], axis=0)
    for sent in (kept, one, two, opposite):
        sent[2 * own :] = flat
    for copy in copies[:3]:
        copy.wait()
    for slot, sent in enumerate((kept, one, two, opposite)):
        at = pl.ds(pl.multiple_of(place[8 + slot] * own, own), own)
        sent[:own] = cost[at] + ph_mult[at] - penalty * consensus[...]
        sent[own : 2 * own] = start[at]
    copies[3].wait()


def run_prepare(place, cost, ph_mult, start, consensus, upper, matrix, blocks):
    group, width = start.shape
    vmem = pl.BlockSpec(memory_space=pltpu.VMEM)
    hbm = pl.BlockSpec(memory_space=pltpu.HBM)
    held = pltpu.VMEM((group, width), jnp.float32)
    state = jax.ShapeDtypeStruct((2 * group // blocks + 8, width), jnp.float32)
    return pl.pallas_call(
        prepare,
        out_shape=(state, state, state, state, jax.ShapeDtypeStruct((TILE, width), jnp.bfloat16)),
        in_specs=[pl.BlockSpec(memory_space=pltpu.SMEM)] + [hbm] * 3 + [vmem] * 2 + [hbm],
        out_specs=(vmem,) * 5,
        scratch_shapes=[held, held, held, pltpu.SemaphoreType.DMA((4,))],
        compiler_params=pltpu.CompilerParams(vmem_limit_bytes=60 * 1024 * 1024),
        cost_estimate=pl.CostEstimate(
            flops=4000000, bytes_accessed=5 * group * width * 4, transcendentals=0
        ),
        name="prepare",
    )(place, cost, ph_mult, start, consensus[None], upper[None], matrix)


def stage(matrix, kept, matrix_out, kept_out, sem):
    copies = [
        pltpu.make_async_copy(matrix, matrix_out, sem.at[0]),
        pltpu.make_async_copy(kept, kept_out, sem.at[1]),
    ]
    for copy in copies:
        copy.start()
    for copy in copies:
        copy.wait()


def run_stage(matrix, kept):
    return pl.pallas_call(
        stage,
        out_shape=tuple(jax.ShapeDtypeStruct(a.shape, a.dtype) for a in (matrix, kept)),
        in_specs=[pl.BlockSpec(memory_space=pltpu.HBM)] * 2,
        out_specs=(pl.BlockSpec(memory_space=pltpu.VMEM),) * 2,
        scratch_shapes=[pltpu.SemaphoreType.DMA((2,))],
        compiler_params=pltpu.CompilerParams(vmem_limit_bytes=8 * 1024 * 1024),
        cost_estimate=pl.CostEstimate(
            flops=4000000, bytes_accessed=2 * matrix.size * 2, transcendentals=0
        ),
        name="stage",
    )(matrix, kept)


def finish(place, p0, p1, p2, p3, back, ph_mult, old, x, mult, z, w, primal, dual):
    blocks, own, _ = back.shape
    width = x.shape[1]
    n_vars = blocks * width
    parts = (p0[...] + p2[...]) + (p1[...] + p3[...])
    total, square = parts[blocks : blocks + 1, :1], parts[blocks + 1 : blocks + 2, :1]
    z_all = parts[:blocks] / total
    primal_sum = square - total * jnp.sum(z_all * z_all, keepdims=True)
    primal[...] = jnp.sqrt(primal_sum / (total * n_vars) + eps)
    gap = z_all - old[...]
    dual[...] = penalty * jnp.sqrt(jnp.sum(gap * gap, keepdims=True) / n_vars + eps)
    mine = lax.broadcasted_iota(jnp.int32, (blocks, 1), 0) == place[8]
    z_own = jnp.sum(jnp.where(mine, z_all, 0.0), axis=0, keepdims=True)
    z[...] = z_own
    for b in range(blocks):
        at = slice(b * own, (b + 1) * own)
        solved = back[b, :, :width]
        x[at] = solved
        mult[at] = back[b, :, width:]
        w[at] = ph_mult[at] + penalty * (solved - z_own)


def run_finish(place, shares, back, ph_mult, old):
    _, _, both = back.shape
    group, width = ph_mult.shape
    vmem = pl.BlockSpec(memory_space=pltpu.VMEM)
    shapes = ((group, width), (group, both - width), (1, width), (group, width), (1, 1), (1, 1))
    return pl.pallas_call(
        finish,
        out_shape=tuple(jax.ShapeDtypeStruct(shape, jnp.float32) for shape in shapes),
        in_specs=[pl.BlockSpec(memory_space=pltpu.SMEM)] + [vmem] * 7,
        out_specs=(vmem,) * 6,
        compiler_params=pltpu.CompilerParams(vmem_limit_bytes=8 * 1024 * 1024),
        cost_estimate=pl.CostEstimate(
            flops=4000000, bytes_accessed=5 * group * width * 4, transcendentals=0
        ),
        name="finish",
    )(place, *shares, back, ph_mult, old)


def local_steps(place, *refs):
    pieces, refs = refs[:24], refs[24:]
    own_a, scale_h, rhs_h, mult_h, weight_h = refs[:5]
    state, (out, parts, old) = refs[5:9], refs[9:12]
    at_v, x_v, w_v, back_v, scale, rhs, mult = refs[12:]
    slots, own, width = x_v.shape
    rows = at_v.shape[1]
    n_piece = rows // TILE
    per_half = n_piece // 2
    first = pl.multiple_of(place[12], 8)

    def tile(p, b, j):
        col = slice(j * TILE, (j + 1) * TILE)
        if b == 0:
            return own_a[pl.ds(pl.multiple_of(place[p], TILE), TILE), col]
        side, q = divmod(p, per_half)
        k = b - 1 if side == 0 else (1, 0, 2)[b - 1]
        return pieces[side * 12 + k * 4 + q][:, col]

    tiles = [(b, j) for b in range(slots) for j in range(width // TILE)]
    for p in range(n_piece):
        at = slice(p * TILE, (p + 1) * TILE)
        there = (pl.ds(first, own), pl.ds(pl.multiple_of(place[p], TILE), TILE))
        scale[:, at] = scale_h[there]
        rhs[:, at] = rhs_h[there]
        mult[:, at] = mult_h[there]
    for b in range(slots):
        x_v[b] = state[b][own : 2 * own]
        old[pl.ds(place[8 + b], 1)] = state[b][2 * own + 1 : 2 * own + 2]

    def turn(p):
        at = slice(p * TILE, (p + 1) * TILE)
        for b, j in tiles:
            var = b * width + j * TILE
            at_v[var : var + TILE, at] = tile(p, b, j).T

    def current():
        return jnp.concatenate([x_v[b] for b in range(slots)], axis=1).astype(jnp.bfloat16)

    def residual(p, xb):
        at = slice(p * TILE, (p + 1) * TILE)
        prod = jnp.dot(xb, at_v[:, at], preferred_element_type=jnp.float32)
        return mult[:, at] + aug_weight * (scale[:, at] * prod - rhs[:, at])

    def weigh(p, xb):
        at = slice(p * TILE, (p + 1) * TILE)
        w_v[:, at] = (scale[:, at] * residual(p, xb)).astype(jnp.bfloat16)

    def add_back(p):
        at = slice(p * TILE, (p + 1) * TILE)
        for b, j in tiles:
            col = slice(j * TILE, (j + 1) * TILE)
            back = jnp.dot(w_v[:, at], tile(p, b, j), preferred_element_type=jnp.float32)
            back_v[b, :, col] = back if p == 0 else back_v[b, :, col] + back

    def move(b, j, back):
        col = slice(j * TILE, (j + 1) * TILE)
        x = x_v[b, :, col]
        grad = state[b][:own, col] + penalty * x + back
        box = state[b][2 * own : 2 * own + 1, col]
        x_v[b, :, col] = jnp.clip(x - step_size * grad, -box, box)

    xb = current()
    for p in range(n_piece):
        turn(p)
        if p > 0:
            add_back(p - 1)
        weigh(p, xb)
    add_back(n_piece - 1)
    for b, j in tiles:
        move(b, j, back_v[b, :, j * TILE : (j + 1) * TILE])

    @pl.loop(1, ITERS)
    def _(i):
        xb = current()
        for p in range(n_piece):
            weigh(p, xb)
        w = w_v[...]
        for b, j in tiles:
            tall = jnp.concatenate([tile(p, b, j) for p in range(n_piece)], axis=0)
            move(b, j, jnp.dot(w, tall, preferred_element_type=jnp.float32))

    share = rows // slots
    xb = current()
    for p in range(n_piece):
        at = place[p]
        inside = pl.ds(pl.multiple_of(width + lax.rem(at, share), TILE), TILE)
        out[lax.div(at, share), :, inside] = residual(p, xb)
    weight = weight_h[pl.ds(first, own), :1]
    square = jnp.zeros((1, 1), jnp.float32)
    for b in range(slots):
        block = place[8 + b]
        x = x_v[b]
        out[block, :, :width] = x
        weighted = weight * x
        parts[pl.ds(block, 1), :] = jnp.sum(weighted, axis=0, keepdims=True)
        square += jnp.sum(weighted * x, keepdims=True)
    total = jnp.sum(weight, axis=0, keepdims=True)
    parts[4:5, :] = jnp.broadcast_to(total, (1, width))
    parts[5:6, :] = jnp.broadcast_to(square, (1, width))
    parts[6:8, :] = jnp.zeros((2, width), jnp.float32)


def run_local(place, mine, theirs, matrix, scale, rhs, mult, weight, state):
    rows, width = matrix.shape
    blocks = len(state)
    own = scale.shape[0] // blocks
    pieces = [piece for block in mine + theirs for piece in block]
    vmem = pl.BlockSpec(memory_space=pltpu.VMEM)
    smem = pl.BlockSpec(memory_space=pltpu.SMEM)
    per_row = pltpu.VMEM((own, rows), jnp.float32)
    return pl.pallas_call(
        local_steps,
        out_shape=(
            jax.ShapeDtypeStruct((blocks, own, width + rows // blocks), jnp.float32),
            jax.ShapeDtypeStruct((8, width), jnp.float32),
            jax.ShapeDtypeStruct((blocks, width), jnp.float32),
        ),
        in_specs=[smem] + [vmem] * (len(pieces) + 5 + blocks),
        out_specs=(vmem,) * 3,
        scratch_shapes=[
            pltpu.VMEM((blocks * width, rows), jnp.bfloat16),
            pltpu.VMEM((blocks, own, width), jnp.float32),
            pltpu.VMEM((own, rows), jnp.bfloat16),
            pltpu.VMEM((blocks, own, width), jnp.float32),
            per_row,
            per_row,
            per_row,
        ],
        compiler_params=pltpu.CompilerParams(vmem_limit_bytes=22 * 1024 * 1024),
        cost_estimate=pl.CostEstimate(
            flops=2 * (2 * ITERS + 1) * own * rows * blocks * width,
            bytes_accessed=2 * blocks * rows * width,
            transcendentals=0,
        ),
        name="local_steps",
    )(place, *pieces, matrix, scale, rhs, mult, weight, *state)


def shift(value, axis, by):
    n = lax.axis_size(axis)
    return lax.ppermute(value, axis, [(i, (i + by) % n) for i in range(n)])


def ring_sum(value, axis):
    return (value + shift(value, axis, 2)) + (shift(value, axis, 1) + shift(value, axis, 3))


def per_device(cons_matrix, row_scale, rhs, cons_mult, cost, ph_mult, start, consensus, upper, prob):
    blocks = lax.axis_size("y")
    me = lax.axis_index("y")
    rows, _ = cons_matrix.shape
    group = start.shape[0]
    own = group // blocks

    c, i, j = ring_place()
    half = rows // 2
    turn = jnp.array([0, 3, 1, 2], jnp.int32)
    near, far = me ^ 1, 3 - me
    place = jnp.concatenate(
        [
            c * half + (i + turn) % RING * TILE,
            (1 - c) * half + (j + turn) % RING * TILE,
            jnp.stack([me, jnp.where(c == 0, near, far), jnp.where(c == 0, far, near), me ^ 2]),
            jnp.stack([me * own]),
        ]
    ).astype(jnp.int32)
    kept, first, opposite, second, far = run_prepare(
        place, cost, ph_mult, start, consensus, upper, cons_matrix, blocks
    )
    mine, theirs = gather_matrix(cons_matrix, far)
    near_matrix, kept = run_stage(cons_matrix, kept)
    state = (kept, send(first, FIRST), send(second, SECOND), send(send(opposite, FIRST), SECOND))

    weight = jnp.broadcast_to(prob[:, None], (group, 128))
    result, parts, old = run_local(
        place, mine, theirs, near_matrix, row_scale, rhs, cons_mult, weight, state
    )

    back = lax.all_to_all(result, "y", 0, 0, tiled=True)
    parts = parts + send(parts, OTHER)
    parts = ring_sum(ring_sum(parts, "x"), "z")
    shares = (parts, shift(parts, "y", 1), shift(parts, "y", 2), shift(parts, "y", 3))
    x, mult_new, z_new, w_new, primal_res, dual_res = run_finish(
        place, shares, back, ph_mult, old
    )
    return (x, mult_new, z_new[0], w_new, primal_res[0, 0], dual_res[0, 0])


def solution(mesh):
    fine = Mesh(mesh.devices.reshape(RING, RING, 2, RING), ALL)
    in_specs = (
        P(None, "y"),
        P(SCEN, None),
        P(SCEN, None),
        P(SCEN, None),
        P(SCEN, "y"),
        P(SCEN, "y"),
        P(SCEN, "y"),
        P("y"),
        P("y"),
        P(SCEN),
    )
    out_specs = (P(SCEN, "y"), P(SCEN, "y"), P("y"), P(SCEN, "y"), P(), P())
    return jax.shard_map(per_device, mesh=fine, in_specs=in_specs, out_specs=out_specs, check_vma=False)
```

```python
import jax
import jax.numpy as jnp
from jax import lax
from jax.experimental import pallas as pl
from jax.experimental.pallas import tpu as pltpu
from jax.sharding import Mesh
from jax.sharding import PartitionSpec as P


ITERS = 8
penalty = 1.0
aug_weight = 1.0
step_size = 0.05
eps = 1e-06


SCEN = ("x", "z", "c")
ALL = ("x", "z", "c", "y")
RING = 4
TILE = 256


def pairs(move):
    def flat(x, z, c, y):
        return ((x * RING + z) * 2 + c) * RING + y

    spots = [
        (x, z, c, y) for x in range(RING) for z in range(RING) for c in range(2) for y in range(RING)
    ]
    return [(flat(*spot), flat(*move(*spot))) for spot in spots]


def along(step):
    def move(x, z, c, y):
        return ((x + step) % RING, z, c, y) if c == 0 else (x, (z + step) % RING, c, y)

    return pairs(move)


FIRST = pairs(lambda x, z, c, y: (x, z, c, y ^ 1 if c == 0 else 3 - y))
SECOND = pairs(lambda x, z, c, y: (x, z, c, 3 - y if c == 0 else y ^ 1))
OTHER = pairs(lambda x, z, c, y: (x, z, 1 - c, y))
UP, DOWN = along(1), along(-1)


def send(value, perm):
    return lax.ppermute(value, ALL, perm)


def ring_place():
    x, z, c = lax.axis_index("x"), lax.axis_index("z"), lax.axis_index("c")
    return c, jnp.where(c == 0, x, z), jnp.where(c == 0, z, x)


def gather_matrix(matrix, far):
    c, i, _ = ring_place()
    half = matrix.shape[0] // 2
    quarter = half // RING
    own = lax.dynamic_slice_in_dim(matrix, c * half + i * quarter, quarter, 0)
    one = send(own, FIRST)
    three = send(one, SECOND)
    two = send(own, SECOND)
    up1, down1 = send(one, UP), send(one, DOWN)
    up3, down3 = send(three, UP), send(three, DOWN)
    up2, down2 = send(two, UP), send(two, DOWN)
    far1 = send(far, FIRST)
    far2 = send(far, SECOND)
    far3 = send(down3, DOWN)
    mine = [[one, up1, down1, far1], [two, up2, down2, far2], [three, up3, down3, far3]]
    theirs = [[send(piece, OTHER) for piece in block] for block in mine]
    return mine, theirs


def prepare(place, cost_h, ph_h, start_h, consensus, upper, matrix, kept, one, opposite, two, far, *scratch):
    cost, ph_mult, start, sem = scratch
    loads = ((cost_h, cost), (ph_h, ph_mult), (start_h, start))
    loads += ((matrix.at[pl.ds(pl.multiple_of(place[3], TILE), TILE)], far),)
    copies = [pltpu.make_async_copy(src, dst, sem.at[k]) for k, (src, dst) in enumerate(loads)]
    for copy in copies:
        copy.start()
    rows, width = kept.shape
    own = (rows - 8) // 2
    flat = jnp.concatenate([upper[...], consensus[...], jnp.zeros((6, width), jnp.float32)], axis=0)
    for sent in (kept, one, two, opposite):
        sent[2 * own :] = flat
    for copy in copies[:3]:
        copy.wait()
    for slot, sent in enumerate((kept, one, two, opposite)):
        at = pl.ds(pl.multiple_of(place[8 + slot] * own, own), own)
        sent[:own] = cost[at] + ph_mult[at] - penalty * consensus[...]
        sent[own : 2 * own] = start[at]
    copies[3].wait()


def run_prepare(place, cost, ph_mult, start, consensus, upper, matrix, blocks):
    group, width = start.shape
    vmem = pl.BlockSpec(memory_space=pltpu.VMEM)
    hbm = pl.BlockSpec(memory_space=pltpu.HBM)
    held = pltpu.VMEM((group, width), jnp.float32)
    state = jax.ShapeDtypeStruct((2 * group // blocks + 8, width), jnp.float32)
    return pl.pallas_call(
        prepare,
        out_shape=(state, state, state, state, jax.ShapeDtypeStruct((TILE, width), jnp.bfloat16)),
        in_specs=[pl.BlockSpec(memory_space=pltpu.SMEM)] + [hbm] * 3 + [vmem] * 2 + [hbm],
        out_specs=(vmem,) * 5,
        scratch_shapes=[held, held, held, pltpu.SemaphoreType.DMA((4,))],
        compiler_params=pltpu.CompilerParams(vmem_limit_bytes=60 * 1024 * 1024),
        cost_estimate=pl.CostEstimate(
            flops=4000000, bytes_accessed=5 * group * width * 4, transcendentals=0
        ),
        name="prepare",
    )(place, cost, ph_mult, start, consensus[None], upper[None], matrix)


def stage(matrix, kept, matrix_out, kept_out, sem):
    copies = [
        pltpu.make_async_copy(matrix, matrix_out, sem.at[0]),
        pltpu.make_async_copy(kept, kept_out, sem.at[1]),
    ]
    for copy in copies:
        copy.start()
    for copy in copies:
        copy.wait()


def run_stage(matrix, kept):
    return pl.pallas_call(
        stage,
        out_shape=tuple(jax.ShapeDtypeStruct(a.shape, a.dtype) for a in (matrix, kept)),
        in_specs=[pl.BlockSpec(memory_space=pltpu.HBM)] * 2,
        out_specs=(pl.BlockSpec(memory_space=pltpu.VMEM),) * 2,
        scratch_shapes=[pltpu.SemaphoreType.DMA((2,))],
        compiler_params=pltpu.CompilerParams(vmem_limit_bytes=8 * 1024 * 1024),
        cost_estimate=pl.CostEstimate(
            flops=4000000, bytes_accessed=2 * matrix.size * 2, transcendentals=0
        ),
        name="stage",
    )(matrix, kept)


def finish(place, p0, p1, p2, p3, back, ph_mult, old, x, mult, z, w, primal, dual):
    blocks, own, _ = back.shape
    width = x.shape[1]
    n_vars = blocks * width
    parts = (p0[...] + p2[...]) + (p1[...] + p3[...])
    total, square = parts[blocks : blocks + 1, :1], parts[blocks + 1 : blocks + 2, :1]
    z_all = parts[:blocks] / total
    primal_sum = square - total * jnp.sum(z_all * z_all, keepdims=True)
    primal[...] = jnp.sqrt(primal_sum / (total * n_vars) + eps)
    gap = z_all - old[...]
    dual[...] = penalty * jnp.sqrt(jnp.sum(gap * gap, keepdims=True) / n_vars + eps)
    mine = lax.broadcasted_iota(jnp.int32, (blocks, 1), 0) == place[8]
    z_own = jnp.sum(jnp.where(mine, z_all, 0.0), axis=0, keepdims=True)
    z[...] = z_own
    for b in range(blocks):
        at = slice(b * own, (b + 1) * own)
        solved = back[b, :, :width]
        x[at] = solved
        mult[at] = back[b, :, width:]
        w[at] = ph_mult[at] + penalty * (solved - z_own)


def run_finish(place, shares, back, ph_mult, old):
    _, _, both = back.shape
    group, width = ph_mult.shape
    vmem = pl.BlockSpec(memory_space=pltpu.VMEM)
    shapes = ((group, width), (group, both - width), (1, width), (group, width), (1, 1), (1, 1))
    return pl.pallas_call(
        finish,
        out_shape=tuple(jax.ShapeDtypeStruct(shape, jnp.float32) for shape in shapes),
        in_specs=[pl.BlockSpec(memory_space=pltpu.SMEM)] + [vmem] * 7,
        out_specs=(vmem,) * 6,
        compiler_params=pltpu.CompilerParams(vmem_limit_bytes=8 * 1024 * 1024),
        cost_estimate=pl.CostEstimate(
            flops=4000000, bytes_accessed=5 * group * width * 4, transcendentals=0
        ),
        name="finish",
    )(place, *shares, back, ph_mult, old)


def local_steps(place, *refs):
    pieces, refs = refs[:24], refs[24:]
    own_a, scale_h, rhs_h, mult_h, weight_h = refs[:5]
    state, (out, parts, old) = refs[5:9], refs[9:12]
    at_v, x_v, w_v, back_v, scale, rhs, mult = refs[12:]
    slots, own, width = x_v.shape
    rows = at_v.shape[1]
    n_piece = rows // TILE
    per_half = n_piece // 2
    first = pl.multiple_of(place[12], 8)

    def tile(p, b, j):
        col = slice(j * TILE, (j + 1) * TILE)
        if b == 0:
            return own_a[pl.ds(pl.multiple_of(place[p], TILE), TILE), col]
        side, q = divmod(p, per_half)
        k = b - 1 if side == 0 else (1, 0, 2)[b - 1]
        return pieces[side * 12 + k * 4 + q][:, col]

    tiles = [(b, j) for b in range(slots) for j in range(width // TILE)]
    for p in range(n_piece):
        at = slice(p * TILE, (p + 1) * TILE)
        there = (pl.ds(first, own), pl.ds(pl.multiple_of(place[p], TILE), TILE))
        scale[:, at] = scale_h[there]
        rhs[:, at] = rhs_h[there]
        mult[:, at] = mult_h[there]
    for b in range(slots):
        x_v[b] = state[b][own : 2 * own]
        old[pl.ds(place[8 + b], 1)] = state[b][2 * own + 1 : 2 * own + 2]

    def turn(p):
        at = slice(p * TILE, (p + 1) * TILE)
        for b, j in tiles:
            var = b * width + j * TILE
            at_v[var : var + TILE, at] = tile(p, b, j).T

    def current():
        return jnp.concatenate([x_v[b] for b in range(slots)], axis=1).astype(jnp.bfloat16)

    def residual(p, xb):
        at = slice(p * TILE, (p + 1) * TILE)
        prod = jnp.dot(xb, at_v[:, at], preferred_element_type=jnp.float32)
        return mult[:, at] + aug_weight * (scale[:, at] * prod - rhs[:, at])

    def weigh(p, xb):
        at = slice(p * TILE, (p + 1) * TILE)
        w_v[:, at] = (scale[:, at] * residual(p, xb)).astype(jnp.bfloat16)

    def add_back(p):
        at = slice(p * TILE, (p + 1) * TILE)
        for b, j in tiles:
            col = slice(j * TILE, (j + 1) * TILE)
            back = jnp.dot(w_v[:, at], tile(p, b, j), preferred_element_type=jnp.float32)
            back_v[b, :, col] = back if p == 0 else back_v[b, :, col] + back

    def move(b, j, back):
        col = slice(j * TILE, (j + 1) * TILE)
        x = x_v[b, :, col]
        grad = state[b][:own, col] + penalty * x + back
        box = state[b][2 * own : 2 * own + 1, col]
        x_v[b, :, col] = jnp.clip(x - step_size * grad, -box, box)

    xb = current()
    for p in range(n_piece):
        turn(p)
        if p > 0:
            add_back(p - 1)
        weigh(p, xb)
    add_back(n_piece - 1)
    for b, j in tiles:
        move(b, j, back_v[b, :, j * TILE : (j + 1) * TILE])

    def step():
        xb = current()
        for p in range(n_piece):
            weigh(p, xb)
        w = w_v[...]
        for b, j in tiles:
            tall = jnp.concatenate([tile(p, b, j) for p in range(n_piece)], axis=0)
            move(b, j, jnp.dot(w, tall, preferred_element_type=jnp.float32))

    for _ in range((ITERS - 1) % 2):
        step()

    @pl.loop(0, (ITERS - 1) // 2)
    def _(i):
        step()
        step()

    share = rows // slots
    xb = current()
    for p in range(n_piece):
        at = place[p]
        inside = pl.ds(pl.multiple_of(width + lax.rem(at, share), TILE), TILE)
        out[lax.div(at, share), :, inside] = residual(p, xb)
    weight = weight_h[pl.ds(first, own), :1]
    square = jnp.zeros((1, 1), jnp.float32)
    for b in range(slots):
        block = place[8 + b]
        x = x_v[b]
        out[block, :, :width] = x
        weighted = weight * x
        parts[pl.ds(block, 1), :] = jnp.sum(weighted, axis=0, keepdims=True)
        square += jnp.sum(weighted * x, keepdims=True)
    total = jnp.sum(weight, axis=0, keepdims=True)
    parts[4:5, :] = jnp.broadcast_to(total, (1, width))
    parts[5:6, :] = jnp.broadcast_to(square, (1, width))
    parts[6:8, :] = jnp.zeros((2, width), jnp.float32)


def run_local(place, mine, theirs, matrix, scale, rhs, mult, weight, state):
    rows, width = matrix.shape
    blocks = len(state)
    own = scale.shape[0] // blocks
    pieces = [piece for block in mine + theirs for piece in block]
    vmem = pl.BlockSpec(memory_space=pltpu.VMEM)
    smem = pl.BlockSpec(memory_space=pltpu.SMEM)
    per_row = pltpu.VMEM((own, rows), jnp.float32)
    return pl.pallas_call(
        local_steps,
        out_shape=(
            jax.ShapeDtypeStruct((blocks, own, width + rows // blocks), jnp.float32),
            jax.ShapeDtypeStruct((8, width), jnp.float32),
            jax.ShapeDtypeStruct((blocks, width), jnp.float32),
        ),
        in_specs=[smem] + [vmem] * (len(pieces) + 5 + blocks),
        out_specs=(vmem,) * 3,
        scratch_shapes=[
            pltpu.VMEM((blocks * width, rows), jnp.bfloat16),
            pltpu.VMEM((blocks, own, width), jnp.float32),
            pltpu.VMEM((own, rows), jnp.bfloat16),
            pltpu.VMEM((blocks, own, width), jnp.float32),
            per_row,
            per_row,
            per_row,
        ],
        compiler_params=pltpu.CompilerParams(vmem_limit_bytes=22 * 1024 * 1024),
        cost_estimate=pl.CostEstimate(
            flops=2 * (2 * ITERS + 1) * own * rows * blocks * width,
            bytes_accessed=2 * blocks * rows * width,
            transcendentals=0,
        ),
        name="local_steps",
    )(place, *pieces, matrix, scale, rhs, mult, weight, *state)


def shift(value, axis, by):
    n = lax.axis_size(axis)
    return lax.ppermute(value, axis, [(i, (i + by) % n) for i in range(n)])


def ring_sum(value, axis):
    return (value + shift(value, axis, 2)) + (shift(value, axis, 1) + shift(value, axis, 3))


def per_device(cons_matrix, row_scale, rhs, cons_mult, cost, ph_mult, start, consensus, upper, prob):
    blocks = lax.axis_size("y")
    me = lax.axis_index("y")
    rows, _ = cons_matrix.shape
    group = start.shape[0]
    own = group // blocks

    c, i, j = ring_place()
    half = rows // 2
    turn = jnp.array([0, 3, 1, 2], jnp.int32)
    near, far = me ^ 1, 3 - me
    place = jnp.concatenate(
        [
            c * half + (i + turn) % RING * TILE,
            (1 - c) * half + (j + turn) % RING * TILE,
            jnp.stack([me, jnp.where(c == 0, near, far), jnp.where(c == 0, far, near), me ^ 2]),
            jnp.stack([me * own]),
        ]
    ).astype(jnp.int32)
    kept, first, opposite, second, far = run_prepare(
        place, cost, ph_mult, start, consensus, upper, cons_matrix, blocks
    )
    mine, theirs = gather_matrix(cons_matrix, far)
    near_matrix, kept = run_stage(cons_matrix, kept)
    state = (kept, send(first, FIRST), send(second, SECOND), send(send(opposite, FIRST), SECOND))

    weight = jnp.broadcast_to(prob[:, None], (group, 128))
    result, parts, old = run_local(
        place, mine, theirs, near_matrix, row_scale, rhs, cons_mult, weight, state
    )

    back = lax.all_to_all(result, "y", 0, 0, tiled=True)
    parts = parts + send(parts, OTHER)
    parts = ring_sum(ring_sum(parts, "x"), "z")
    shares = (parts, shift(parts, "y", 1), shift(parts, "y", 2), shift(parts, "y", 3))
    x, mult_new, z_new, w_new, primal_res, dual_res = run_finish(
        place, shares, back, ph_mult, old
    )
    return (x, mult_new, z_new[0], w_new, primal_res[0, 0], dual_res[0, 0])


def solution(mesh):
    fine = Mesh(mesh.devices.reshape(RING, RING, 2, RING), ALL)
    in_specs = (
        P(None, "y"),
        P(SCEN, None),
        P(SCEN, None),
        P(SCEN, None),
        P(SCEN, "y"),
        P(SCEN, "y"),
        P(SCEN, "y"),
        P("y"),
        P("y"),
        P(SCEN),
    )
    out_specs = (P(SCEN, "y"), P(SCEN, "y"), P("y"), P(SCEN, "y"), P(), P())
    return jax.shard_map(per_device, mesh=fine, in_specs=in_specs, out_specs=out_specs, check_vma=False)
```
